32 devices in a mesh: group: 2 (over x), tp: 4 (over z), dp: 4 (over y, core).
Axes of the slice: x: 2, y: 2, z: 4, core: 2. Of those that a mesh axis runs over, the one named last changes fastest.
Arguments:
- image_slots: bfloat16 [128, 8192], P(('group', 'tp'), 'dp'), may hold values from -6 to 6
- image_cot: bfloat16 [128, 8192], P(('group', 'tp'), 'dp'), may hold values from -6 to 6
- text_rows: bfloat16 [64, 8192], P(('group', 'tp'), 'dp'), may hold values from -6 to 6
- text_cot: bfloat16 [64, 8192], P(('group', 'tp'), 'dp'), may hold values from -6 to 6
- destination: int32 [64, 1], P(('group', 'tp')), may hold values from 0 to 1; in each aligned block of 8 rows (0 to 7, 8 to 15, ...) at most 8 rows name the same one
- text_count: int32 [8], P(('group', 'tp')), may hold values from 1 to 8, 48 in all
- w_gate: bfloat16 [8192, 14336], P('dp', 'tp'), may hold values from -0.0625 to 0.0625
- w_up: bfloat16 [8192, 14336], P('dp', 'tp'), may hold values from -0.0625 to 0.0625
- w_down: bfloat16 [14336, 8192], P('tp', 'dp'), may hold values from -0.046875 to 0.046875
Outputs:
- image_grad: bfloat16 [64, 8192], P(('group', 'tp'), 'dp')
- text_grad: bfloat16 [64, 8192], P(('group', 'tp'), 'dp')
The draws below stay inside these ranges and needn't reach their ends.
Inputs may be any that keep to these rules, and one draw needn't show every extreme that they name: In the rows of one block of 8 rows no group is named more than 8 times, and some block names one group exactly 8 times; destination[i] decides which slot of image_slots and image_cot holds row i. Each block of 8 text rows has text_count live rows first; some block is full.
All inputs are finite; a program needn't handle non-finite values.
Results may differ from the reference program's by a relative error of at most 0.025.
Values may be sent and summed in bfloat16 or wider, within the bound.
No kernel may reach another device: no remote copies, remote signals or barrier semaphores. Data moves between devices by JAX's collectives and lax.ppermute only.
A program may use at most 128 MiB of HBM per device.

```python
import math
import jax
import jax.numpy as jnp
import numpy as np
from jax import lax

D = 8192
FF = 14336
IMG_DEV = 8
TXT_DEV = 8
CAP = 8
SLOTS = 128
IMG_ROWS = 64
TXT_ROWS = 64
N_GROUP = 2
N_TP = 4
N_DP = 4


def block_scale(stream_key, shape, cuts, least, high):
    factor_of = 1.0
    for dim, blocks in cuts:
        steps = jax.random.uniform(jax.random.fold_in(jax.random.fold_in(stream_key, 6), dim), (blocks,), jnp.float32, least / len(cuts), high / len(cuts))
        factor_of = factor_of * jnp.repeat(jnp.exp(steps), shape[dim] // blocks).reshape((-1,) + (1,) * (len(shape) - 1 - dim))
    return factor_of


def split_up(amount, total, most, slope):
    portions = [(1 << 20) // math.isqrt(grade ** slope) + 1 for grade in range(2, amount + 1)]
    surplus, given = total - most - (amount - 1), [1] * (amount - 1)
    while surplus > 0:
        movable = [i for i in range(amount - 1) if given[i] < most]
        whole, left = sum([portions[i] for i in movable]), surplus
        for i in movable:
            extra = min(most - given[i], max(1, left * portions[i] // whole), surplus)
            given[i] = given[i] + extra
            surplus = surplus - extra
    return np.array([most] + given)


def ragged(stream_key, count, total, most, slope):
    if count == 2:
        one = jax.random.randint(stream_key, (), max(1, total - most), min(most, total - 1) + 1)
        return jnp.stack([one, total - one])
    sizes = jnp.asarray(split_up(count, total, most, slope), jnp.int32)
    couples = (count - 1) // 2
    donor, taker = sizes[1:1 + 2 * couples:2], sizes[2:2 + 2 * couples:2]
    slack = jnp.minimum(donor - 1, most - taker)
    shifted = jax.random.randint(jax.random.fold_in(stream_key, 1), (couples,), 0, 1 << 20) % (slack + 1)
    sizes = sizes.at[1:1 + 2 * couples:2].set(donor - shifted).at[2:2 + 2 * couples:2].set(taker + shifted)
    return sizes[jax.random.permutation(jax.random.fold_in(stream_key, 2), count)]


def shared_out(rng, own, number, rows, number_of, top, bound, lean):
    sequence = jax.random.permutation(rng, number_of)
    packed, usual = load_shares(number_of, rows * top, bound, lean, True), load_shares(number_of, rows * top, bound, lean, False)
    places = jnp.arange(number_of)

    def named(tallies, rotation):
        used = int((tallies > 0).sum())
        fixed = max(1, used // 4)
        shifted = fixed + (places - fixed + rotation * (used - fixed)) % max(1, number_of - fixed)
        return jnp.zeros((number_of,), jnp.int32).at[sequence[jnp.where(places < fixed, places, shifted)]].set(jnp.asarray(tallies, jnp.int32))

    tallies = jnp.where(number % 4 == 0, named(packed, number // 4), named(usual, number - number // 4 - 1))
    mixed = jax.random.permutation(jax.random.fold_in(own, 3), number_of)
    source_of, receiver = mixed[0:number_of // 2 * 2:2], mixed[1:number_of // 2 * 2:2]
    margin = jnp.minimum(tallies[source_of] - 1, bound - tallies[receiver]) // 2
    margin = jnp.where((source_of == sequence[0]) | (receiver == sequence[0]) | (tallies[receiver] == 0), 0, jnp.maximum(margin, 0))
    shifted = jax.random.randint(jax.random.fold_in(own, 4), (number_of // 2,), 0, 1 << 20) % (margin + 1)
    tallies = tallies.at[source_of].add(-shifted).at[receiver].add(shifted)
    labels = jnp.searchsorted(jnp.cumsum(tallies), jnp.arange(rows * top), side="right").astype(jnp.int32)
    grid = labels.reshape(top, rows).T
    grid = grid[jax.random.permutation(jax.random.fold_in(own, 1), rows)]
    rotation = jax.random.randint(jax.random.fold_in(own, 2), (rows, 1), 0, top)
    return jnp.take_along_axis(grid, (jnp.arange(top)[None, :] + rotation) % top, axis=1)


def load_shares(number_of, total, most, skew, full):
    weights = [(1 << 20) // math.isqrt(grade ** skew) + 1 for grade in range(1, number_of + 1)]
    largest = most if full else min(most, max(-(-total // number_of), total * weights[0] // sum(weights)))
    least = 1 if total - largest >= number_of - 1 else 0
    given, spare = [largest] + [least] * (number_of - 1), total - largest - least * (number_of - 1)
    while spare > 0:
        movable = [i for i in range(1, number_of) if given[i] < largest] or [i for i in range(1, number_of) if given[i] < most]
        pool, budget = sum([weights[i] for i in movable]), spare
        for i in movable:
            addition = min(most - given[i], max(1, budget * weights[i] // pool), spare)
            given[i] = given[i] + addition
            spare = spare - addition
    return np.array(given)


def centred(key, extent, deviation, reach, pieces=(), kind=jnp.bfloat16):
    drawn = deviation * jax.random.normal(key, extent, jnp.float32)
    if pieces:
        drawn = drawn * block_scale(key, extent, pieces, -0.22, 0.18)
    return jnp.clip(drawn, -reach, reach).astype(kind)


def setup_inputs(seed: int = 0) -> dict:
    streams_of = jax.random.split(jax.random.key(seed), 10)
    image_slots = centred(streams_of[0], (SLOTS, D), 1.0, 6.0, ((0, 8), (1, 4)))
    image_cot = centred(streams_of[1], (SLOTS, D), 1.0, 6.0, ((0, 8), (1, 4)))
    text_rows = centred(streams_of[2], (TXT_ROWS, D), 1.0, 6.0, ((0, 8), (1, 4)))
    text_cot = centred(streams_of[3], (TXT_ROWS, D), 1.0, 6.0, ((0, 8), (1, 4)))
    destination_keys = jax.random.split(jax.random.fold_in(streams_of[4], 1), IMG_ROWS // IMG_DEV)
    destination_turns = jax.random.permutation(jax.random.fold_in(streams_of[4], 3), IMG_ROWS // IMG_DEV)
    destination = jax.vmap(lambda own, number: shared_out(jax.random.fold_in(streams_of[4], 2), own, number, IMG_DEV, N_GROUP, 1, CAP, 2))(destination_keys, destination_turns).reshape((IMG_ROWS, 1))
    text_count = ragged(streams_of[5], N_GROUP * N_TP, 3 * TXT_DEV * N_GROUP * N_TP // 4, TXT_DEV, 2).astype(jnp.int32)
    w_gate = centred(streams_of[6], (D, FF), D ** -0.5, 0.0625, ((0, 4), (1, 4)))
    w_up = centred(streams_of[7], (D, FF), D ** -0.5, 0.0625, ((0, 4), (1, 4)))
    w_down = centred(streams_of[8], (FF, D), FF ** -0.5, 0.046875, ((0, 4), (1, 4)))
    return {"image_slots": image_slots, "image_cot": image_cot, "text_rows": text_rows, "text_cot": text_cot, "destination": destination, "text_count": text_count, "w_gate": w_gate, "w_up": w_up, "w_down": w_down}


def rounded(value):
    return lax.optimization_barrier(value.astype(jnp.bfloat16)).astype(jnp.float32)


def split_features(left, right, parts, transpose_right):
    width = left.shape[1] // parts
    if transpose_right:
        total = jnp.zeros((left.shape[0], right.shape[0]), jnp.float32)
    else:
        total = jnp.zeros((left.shape[0], right.shape[1]), jnp.float32)

    def add_block(index, carry):
        start = (index * width).astype(jnp.int32)
        piece = lax.dynamic_slice_in_dim(left, start, width, 1)
        if transpose_right:
            other = lax.dynamic_slice_in_dim(right, start, width, 1)
            term = lax.dot_general(piece, other, (((1,), (1,)), ((), ())), preferred_element_type=jnp.float32)
        else:
            other = lax.dynamic_slice_in_dim(right, start, width, 0)
            term = jnp.dot(piece, other, preferred_element_type=jnp.float32)
        return carry + rounded(term)

    return lax.fori_loop(0, parts, add_block, total)


def split_hidden(dgate, dup, w_gate, w_up, parts):
    width = dgate.shape[1] // parts
    total = jnp.zeros((dgate.shape[0], w_gate.shape[0]), jnp.float32)

    def add_block(index, carry):
        start = (index * width).astype(jnp.int32)
        gate_piece = lax.dynamic_slice_in_dim(dgate, start, width, 1)
        up_piece = lax.dynamic_slice_in_dim(dup, start, width, 1)
        gate_weight = lax.dynamic_slice_in_dim(w_gate, start, width, 1)
        up_weight = lax.dynamic_slice_in_dim(w_up, start, width, 1)
        term = lax.dot_general(gate_piece, gate_weight, (((1,), (1,)), ((), ())), preferred_element_type=jnp.float32)
        term = term + lax.dot_general(up_piece, up_weight, (((1,), (1,)), ((), ())), preferred_element_type=jnp.float32)
        return carry + rounded(term)

    return lax.fori_loop(0, parts, add_block, total)


def row_grads(rows, cots, w_gate, w_up, w_down):
    gate = split_features(rows, w_gate, N_DP, False)
    up = split_features(rows, w_up, N_DP, False)
    back = split_features(cots, w_down, N_DP, True)
    sigmoid_gate = jax.nn.sigmoid(gate)
    dgate = (back * up * sigmoid_gate * (1.0 + gate * (1.0 - sigmoid_gate))).astype(jnp.bfloat16)
    dup = (back * gate * sigmoid_gate).astype(jnp.bfloat16)
    total = split_hidden(dgate, dup, w_gate, w_up, N_TP)
    return total.astype(jnp.bfloat16)


def reference(image_slots, image_cot, text_rows, text_cot, destination, text_count, w_gate, w_up, w_down):
    blocks = destination[:, 0].astype(jnp.int32).reshape(N_GROUP * N_TP, IMG_DEV)
    same = blocks[:, :, None] == blocks[:, None, :]
    position = jnp.arange(IMG_DEV, dtype=jnp.int32)
    earlier = position[None, :] < position[:, None]
    rank = jnp.sum((same & earlier[None, :, :]).astype(jnp.int32), axis=2)
    source = jnp.arange(N_GROUP * N_TP, dtype=jnp.int32)
    source_group = source // N_TP
    source_tp = source % N_TP
    slot = ((blocks * N_TP + source_tp[:, None]) * N_GROUP + source_group[:, None]) * CAP + rank
    slot = slot.reshape(-1).astype(jnp.int32)
    image_in = jnp.take(image_slots, slot, axis=0)
    image_back = jnp.take(image_cot, slot, axis=0)
    image_grad = row_grads(image_in, image_back, w_gate, w_up, w_down)
    text_grad = row_grads(text_rows, text_cot, w_gate, w_up, w_down)
    within = jnp.arange(TXT_ROWS, dtype=jnp.int32) % TXT_DEV
    limit = jnp.repeat(text_count.astype(jnp.int32), TXT_DEV)
    live = (within < limit)[:, None]
    text_grad = jnp.where(live, text_grad, jnp.zeros_like(text_grad))
    return image_grad, text_grad
```

```python
import jax
import jax.numpy as jnp
from jax import lax
from jax.sharding import PartitionSpec as P

F32 = jnp.float32
BF16 = jnp.bfloat16
DIRECT = 4


def shifted(value, axis, shift):
    size = lax.axis_size(axis)
    return lax.ppermute(value, axis, [(i, (i + shift) % size) for i in range(size)])


def swapped(value, axis, bit):
    size = lax.axis_size(axis)
    return lax.ppermute(value, axis, [(i, i ^ bit) for i in range(size)])


def bits_of(size):
    return [1 << i for i in range(size.bit_length() - 1)]


def by_xor(blocks, index):
    for bit in bits_of(len(blocks)):
        flip = (index & bit) != 0
        blocks = [jnp.where(flip, blocks[j ^ bit], blocks[j]) for j in range(len(blocks))]
    return blocks


def gather_rows(value, axis):
    size = lax.axis_size(axis)
    if size > DIRECT:
        full = lax.all_gather(value, axis, axis=0, tiled=True)
        return jnp.split(full, size, axis=0)
    return [value] + [shifted(value, axis, k) for k in range(1, size)]


def scatter_rows(blocks, axis):
    size = lax.axis_size(axis)
    if size > DIRECT:
        joined = jnp.concatenate([b.astype(BF16) for b in blocks], axis=0)
        return lax.psum_scatter(joined, axis, scatter_dimension=0, tiled=True).astype(F32)
    total = blocks[0]
    for k in range(1, size):
        total = total + shifted(blocks[k].astype(BF16), axis, -k).astype(F32)
    return total


def halve(blocks, axis):
    size = lax.axis_size(axis)
    for bit in bits_of(size):
        count = len(blocks)
        keep = blocks[0::2]
        give = blocks[1::2]
        sent = jnp.concatenate([b.astype(BF16) for b in give], axis=0)
        got = jnp.split(swapped(sent, axis, bit), count // 2, axis=0)
        blocks = [a.astype(F32) + b.astype(F32) for a, b in zip(keep, got)]
    return blocks[0]


def double(value, axis):
    size = lax.axis_size(axis)
    blocks = [value]
    for bit in reversed(bits_of(size)):
        sent = jnp.concatenate(blocks, axis=0)
        got = jnp.split(swapped(sent, axis, bit), len(blocks), axis=0)
        blocks = [b for pair in zip(blocks, got) for b in pair]
    return blocks


def to_blocks(rows, count):
    return jnp.split(rows, count, axis=0)


def language_grads(image, text, w_gate, w_up, w_down):
    parts = lax.axis_size("dp")
    index = lax.axis_index("dp")
    feat = w_gate.shape[0]
    text_all = gather_rows(text, "tp")
    image_all = gather_rows(image, "tp")
    image_dev = image.shape[0]
    tps = len(image_all)
    rows = jnp.concatenate([b for pair in zip(image_all, text_all) for b in pair], axis=0)
    rows = jnp.concatenate(by_xor(to_blocks(rows, parts), index), axis=0)
    inputs_part = rows[:, :feat]
    cot_part = rows[:, feat:]
    back = lax.dot_general(cot_part, w_down, (((1,), (1,)), ((), ())), preferred_element_type=F32)
    back = halve(to_blocks(back, parts), "dp")
    gate = jnp.dot(inputs_part, w_gate, preferred_element_type=F32)
    gate = halve(to_blocks(gate, parts), "dp")
    up = jnp.dot(inputs_part, w_up, preferred_element_type=F32)
    up = halve(to_blocks(up, parts), "dp")
    sigmoid_gate = jax.nn.sigmoid(gate)
    dgate = (back * up * sigmoid_gate * (1.0 + gate * (1.0 - sigmoid_gate))).astype(BF16)
    dup = (back * gate * sigmoid_gate).astype(BF16)
    hidden = dgate.shape[1]
    both = double(jnp.concatenate([dgate, dup], axis=1), "dp")
    both = jnp.concatenate(both, axis=0)
    terms = lax.dot_general(both[:, :hidden], w_gate, (((1,), (1,)), ((), ())), preferred_element_type=F32)
    terms = terms + lax.dot_general(both[:, hidden:], w_up, (((1,), (1,)), ((), ())), preferred_element_type=F32)
    terms = jnp.concatenate(by_xor(to_blocks(terms, parts), index), axis=0)
    return scatter_rows(to_blocks(terms, tps), "tp")


def exchanged(both, capacity):
    groups = lax.axis_size("group")
    if groups != 2:
        arrived = lax.all_to_all(both, "group", split_axis=0, concat_axis=0, tiled=True)
        return arrived, jnp.int32(0)
    mine = lax.axis_index("group")
    first = both[:capacity]
    second = both[capacity:]
    own = jnp.where(mine == 0, first, second)
    give = jnp.where(mine == 0, second, first)
    return jnp.concatenate([own, swapped(give, "group", 1)], axis=0), mine


def per_device(
    image_slots, image_cot, text_rows, text_cot, destination, text_count, w_gate, w_up, w_down
):
    groups = lax.axis_size("group")
    slot_dev = image_slots.shape[0]
    capacity = slot_dev // groups
    image_dev = destination.shape[0]
    text_dev = text_rows.shape[0]
    text_both = jnp.concatenate([text_rows, text_cot], axis=1)
    both = jnp.concatenate([image_slots, image_cot], axis=1)
    arrived, first = exchanged(both, capacity)
    target = destination[:, 0]
    position = lax.broadcasted_iota(jnp.int32, (image_dev, image_dev), 0)
    other = lax.broadcasted_iota(jnp.int32, (image_dev, image_dev), 1)
    same = (target[:, None] == target[None, :]) & (other < position)
    rank = jnp.sum(same.astype(jnp.int32), axis=1)
    column = jnp.bitwise_xor(target, first) * capacity + rank
    slot_index = lax.broadcasted_iota(jnp.int32, (image_dev, slot_dev), 1)
    select = (column[:, None] == slot_index).astype(BF16)
    picked = jnp.dot(select, arrived, preferred_element_type=F32).astype(BF16)
    grads = language_grads(picked, text_both, w_gate, w_up, w_down)
    image_grad = grads[:image_dev].astype(BF16)
    text_part = grads[image_dev:].astype(BF16)
    live = lax.broadcasted_iota(jnp.int32, (text_dev, 1), 0) < text_count[0]
    text_grad = jnp.where(live, text_part, jnp.zeros_like(text_part))
    return (image_grad, text_grad)


def solution(mesh):
    placed = (
        P(("group", "tp"), "dp"),
        P(("group", "tp"), "dp"),
        P(("group", "tp"), "dp"),
        P(("group", "tp"), "dp"),
        P(("group", "tp"), None),
        P(("group", "tp")),
        P("dp", "tp"),
        P("dp", "tp"),
        P("tp", "dp"),
    )
    return jax.shard_map(
        per_device,
        mesh=mesh,
        in_specs=placed,
        out_specs=(P(("group", "tp"), "dp"), P(("group", "tp"), "dp")),
        check_vma=False,
    )
```

```python
import jax
import jax.numpy as jnp
from jax import lax
from jax.experimental import pallas as pl
from jax.experimental.pallas import tpu as pltpu
from jax.sharding import PartitionSpec as P


F32 = jnp.float32
BF16 = jnp.bfloat16
DIRECT = 4
LIMIT = 6 << 20
CHUNKS = 4
NT = (((1,), (1,)), ((), ()))


def in_vmem(value):
    return pltpu.with_memory_space_constraint(value, pltpu.VMEM)


def in_hbm(value):
    return pltpu.with_memory_space_constraint(value, pltpu.HBM)


def array(shape, dtype):
    return jax.ShapeDtypeStruct(shape, dtype)


def call(kernel, out_shape, values, kinds, flops=0, scratch=(), extra=0):
    memory = {"S": pltpu.SMEM, "V": pltpu.VMEM, "H": pltpu.HBM, "A": pl.ANY}
    values = [in_hbm(v) if kind == "H" else v for v, kind in zip(values, kinds)]
    nbytes = sum(v.size * v.dtype.itemsize for v in values)
    return pl.pallas_call(
        kernel,
        out_shape=out_shape,
        in_specs=[pl.BlockSpec(memory_space=memory[kind]) for kind in kinds],
        out_specs=jax.tree.map(lambda _: pl.BlockSpec(memory_space=pltpu.VMEM), out_shape),
        scratch_shapes=list(scratch),
        compiler_params=pltpu.CompilerParams(vmem_limit_bytes=LIMIT + extra),
        cost_estimate=pl.CostEstimate(flops=max(flops, nbytes), transcendentals=0, bytes_accessed=nbytes),
    )(*values)


def swapped(value, axis, bit):
    size = lax.axis_size(axis)
    return lax.ppermute(value, axis, [(i, i ^ bit) for i in range(size)])


def bits_of(size):
    return [1 << i for i in range(size.bit_length() - 1)]


def blocks_of(rows, count):
    return jnp.split(rows, count, axis=0)


def by_xor(blocks, bits):
    for n, bit in enumerate(bits_of(len(blocks))):
        flip = bits[n : n + 1, :1] != 0
        blocks = [jnp.where(flip, blocks[j ^ bit], blocks[j]) for j in range(len(blocks))]
    return blocks


def gather_rows(value, axis):
    size = lax.axis_size(axis)
    if size > DIRECT:
        return blocks_of(lax.all_gather(value, axis, axis=0, tiled=True), size)
    blocks = [value]
    for k in range(1, size):
        blocks.append(swapped(value, axis, k))
    return blocks


def scatter_rows(blocks, axis):
    size = lax.axis_size(axis)
    if size > DIRECT:
        joined = jnp.concatenate([b.astype(BF16) for b in blocks], axis=0)
        return lax.psum_scatter(joined, axis, scatter_dimension=0, tiled=True).astype(F32)
    total = blocks[0]
    sent = [b.astype(BF16) for b in blocks[1:]]
    for k in range(1, size):
        got = swapped(sent[k - 1], axis, k)
        total = total + got.astype(F32)
    return total


def copies_of(source, target, sems, count=CHUNKS):
    step = source.shape[0] // count
    rows = [pl.ds(i * step, step) for i in range(count)]
    return [pltpu.make_async_copy(source.at[r], target.at[r], sems.at[i]) for i, r in enumerate(rows)]


def loaded(weight, after):
    def kernel(w_ref, after_ref, out_ref, sems):
        copies = copies_of(w_ref, out_ref, sems)
        for copy in copies:
            copy.start()
        for copy in copies:
            copy.wait()

    out = pltpu.VMEM(weight.shape, weight.dtype)
    return call(kernel, out, (weight, after), "HA", int(4e9), [pltpu.SemaphoreType.DMA((CHUNKS,))])


def prepare(flags, image_slots, image_cot, text_rows, text_cot, capacity):
    slots, feat = image_slots.shape
    two = slots == 2 * capacity
    text_dev = text_rows.shape[0]
    kept = capacity if two else slots

    def kernel(flags_ref, slots_ref, cot_ref, text_ref, text_cot_ref, own_ref, give_ref, text_out_ref, bits_ref, sems):
        pairs = []
        for at, image, text in ((pl.ds(0, feat), slots_ref, text_ref), (pl.ds(feat, feat), cot_ref, text_cot_ref)):
            start = flags_ref[0] * capacity if two else 0
            pairs.append((image.at[pl.ds(start, kept)], own_ref.at[:, at]))
            pairs.append((text, text_out_ref.at[:, at]))
            if two:
                pairs.append((image.at[pl.ds(capacity - start, kept)], give_ref.at[:, at]))
        copies = [pltpu.make_async_copy(a, b, sems.at[i]) for i, (a, b) in enumerate(pairs)]
        for copy in copies:
            copy.start()
        row = lax.broadcasted_iota(jnp.int32, bits_ref.shape, 0)
        index = jnp.full(bits_ref.shape, flags_ref[1], jnp.int32)
        bits_ref[...] = lax.shift_right_logical(index, row) & 1
        if not two:
            give_ref[...] = jnp.zeros_like(give_ref)
        for copy in copies:
            copy.wait()

    given = capacity if two else 8
    out = (
        array((kept, 2 * feat), BF16),
        array((given, 2 * feat), BF16),
        array((text_dev, 2 * feat), BF16),
        array((8, 128), jnp.int32),
    )
    values = (flags, image_slots, image_cot, text_rows, text_cot)
    return call(kernel, out, values, "SHHHH", 0, [pltpu.SemaphoreType.DMA((6,))])


def pick(flags, own, got, destination, capacity, two):
    rows = destination.shape[0]
    slots = own.shape[0] * (2 if two else 1)
    width = own.shape[1]

    def kernel(flags_ref, target_ref, own_ref, got_ref, out_ref):
        target = [target_ref[i] for i in range(rows)]
        first = flags_ref[0] if two else 0
        position = lax.broadcasted_iota(jnp.int32, (rows, slots), 0)
        index = lax.broadcasted_iota(jnp.int32, (rows, slots), 1)
        column = jnp.zeros((rows, slots), jnp.int32)
        for i in range(rows):
            rank = jnp.int32(0)
            for j in range(i):
                rank = rank + (target[j] == target[i]).astype(jnp.int32)
            slot = jnp.bitwise_xor(target[i], first) * capacity + rank
            column = jnp.where(position == i, slot, column)
        select = jnp.where(column == index, 1.0, 0.0).astype(BF16)
        if two:
            half = own_ref.shape[0]
            out = jnp.dot(select[:, :half], own_ref[...], preferred_element_type=F32)
            out = out + jnp.dot(select[:, half:], got_ref[...], preferred_element_type=F32)
        else:
            out = jnp.dot(select, own_ref[...], preferred_element_type=F32)
        out_ref[...] = out.astype(BF16)

    return call(kernel, array((rows, width), BF16), (flags, destination, own, got), "SSVV")


def step_of(width):
    for step in (896, 512, 256):
        if width % step == 0:
            return step
    return 128


def split_store(out, keep_ref, give_ref, to, part):
    for i in range(out.shape[0] // part // 2):
        kept = out[2 * i * part : (2 * i + 1) * part]
        given = out[(2 * i + 1) * part : (2 * i + 2) * part]
        keep_ref[i * part : (i + 1) * part, to] = kept
        give_ref[i * part : (i + 1) * part, to] = given.astype(BF16)


def low_part(weight):
    return -(-weight.shape[0] // 256) * 128


def forward_in(x, w_gate, w_up, parts):
    rows = x.shape[0]
    width = w_gate.shape[1]
    step = step_of(width)
    count = width // step

    def kernel(x_ref, gate_ref, up_hbm, keep_ref, give_ref, up_ref, up_sems):
        columns = [pl.ds(j * step, step) for j in range(count)]
        ups = [pltpu.make_async_copy(up_hbm.at[:, c], up_ref.at[:, c], up_sems.at[j]) for j, c in enumerate(columns)]
        for copy in ups:
            copy.start()
        for n, w_ref in enumerate((gate_ref, up_ref)):
            for j, at in enumerate(columns):
                if n == 1:
                    ups[j].wait()
                out = jnp.dot(x_ref[...], w_ref[:, at], preferred_element_type=F32)
                split_store(out, keep_ref, give_ref, pl.ds(n * width + j * step, step), rows // parts)

    out = (
        array((rows // 2, 2 * width), F32),
        array((rows // 2, 2 * width), BF16),
        pltpu.VMEM(w_up.shape, w_up.dtype),
    )
    values = (x, in_vmem(w_gate), w_up)
    scratch = [pltpu.SemaphoreType.DMA((count,))]
    return call(kernel, out, values, "VVH", 4 * rows * w_up.size, scratch)


def forward_back(x, weight, kept, after, parts, first, width):
    rows = x.shape[0]
    step = 256 if width % 256 == 0 else 128
    count = width // step

    def kernel(x_ref, w_ref, after_ref, keep_ref, give_ref, w_buf, sems):
        copies = copies_of(w_ref.at[pl.ds(first, width)], w_buf, sems, count)
        for copy in copies:
            copy.start()
        for j in range(count):
            at = pl.ds(j * step, step)
            copies[j].wait()
            out = lax.dot_general(x_ref[...], w_buf[at, :], NT, preferred_element_type=F32)
            split_store(out, keep_ref, give_ref, at, rows // parts)

    out = (array((rows // 2, width), F32), array((rows // 2, width), BF16))
    scratch = [pltpu.VMEM((width, weight.shape[1]), weight.dtype), pltpu.SemaphoreType.DMA((count,))]
    extra = width * weight.shape[1] * 2
    values = (x, weight, *[w for w in kept[:0]], after)
    return call(kernel, out, values, "VHA", 2 * rows * width * weight.shape[1], scratch, extra)


def halve_first(give, keep, axis):
    half = lax.axis_size(axis) // 2
    got = blocks_of(swapped(give, axis, 1), half)
    return [a + b.astype(F32) for a, b in zip(blocks_of(keep, half), got)]


def sent_rows(blocks):
    return jnp.concatenate([b.astype(BF16) for b in blocks[1::2]], axis=0)


def halve_rest(blocks, axis, sent):
    for bit in bits_of(lax.axis_size(axis))[1:]:
        got = blocks_of(swapped(sent, axis, bit), len(blocks) // 2)
        blocks = [a + b.astype(F32) for a, b in zip(blocks[0::2], got)]
        sent = sent_rows(blocks) if len(blocks) > 1 else None
    return blocks[0]


def double(value, axis):
    pieces = [value]
    for bit in reversed(bits_of(lax.axis_size(axis))):
        got = blocks_of(swapped(jnp.concatenate(pieces, axis=0), axis, bit), len(pieces))
        pieces = [b for pair in zip(pieces, got) for b in pair]
    return pieces


def backward(x, w_gate, w_up):
    rows, _ = x.shape
    feat, hidden = w_gate.shape
    step = min(step_of(feat), 512)

    def kernel(x_ref, gate_ref, up_ref, out_ref):
        for j in range(feat // step):
            at = pl.ds(j * step, step)
            out = lax.dot_general(x_ref[:, :hidden], gate_ref[at, :], NT, preferred_element_type=F32)
            out = out + lax.dot_general(x_ref[:, hidden:], up_ref[at, :], NT, preferred_element_type=F32)
            out_ref[:, at] = out

    values = (x, in_vmem(w_gate), in_vmem(w_up))
    return call(kernel, array((rows, feat), F32), values, "VVV", 4 * rows * w_gate.size)


def per_device(
    image_slots, image_cot, text_rows, text_cot, destination, text_count, w_gate, w_up, w_down
):
    groups = lax.axis_size("group")
    parts = lax.axis_size("dp")
    capacity = image_slots.shape[0] // groups
    image_dev = destination.shape[0]
    feat, hidden = w_gate.shape
    two = groups == 2
    flags = jnp.stack([lax.axis_index("group"), lax.axis_index("dp")]).astype(jnp.int32)
    own, give, text, bits = prepare(flags, image_slots, image_cot, text_rows, text_cot, capacity)
    if two:
        got = swapped(give, "group", 1)
    else:
        own = lax.all_to_all(own, "group", split_axis=0, concat_axis=0, tiled=True)
        got = give
    text_all = gather_rows(text, "tp")
    picked = pick(flags, own, got, destination.reshape(image_dev), capacity, two)
    image_all = gather_rows(picked, "tp")
    w_gate = loaded(w_gate, picked)
    rows = jnp.concatenate([b for pair in zip(image_all, text_all) for b in pair], axis=0)
    rows = jnp.concatenate(by_xor(blocks_of(rows, parts), bits), axis=0)

    keep, give, w_up = forward_in(rows[:, :feat], w_gate, w_up, parts)
    low = low_part(w_down)
    both = halve_first(give, keep, "dp")
    cot = rows[:, feat:]
    sent = sent_rows(both)
    keep_low, give_low = forward_back(cot, w_down, (w_gate, w_up), give, parts, 0, low)
    keep_high, give_high = forward_back(cot, w_down, (w_gate, w_up), sent, parts, low, hidden - low)
    both = halve_rest(both, "dp", sent)
    keep = jnp.concatenate([keep_low, keep_high], axis=1)
    give = jnp.concatenate([give_low, give_high], axis=1)
    back = halve_first(give, keep, "dp")
    back = halve_rest(back, "dp", sent_rows(back))

    gate = both[:, :hidden]
    up = both[:, hidden:]
    sigmoid_gate = jax.nn.sigmoid(gate)
    dgate = (back * up * sigmoid_gate * (1.0 + gate * (1.0 - sigmoid_gate))).astype(BF16)
    dup = (back * gate * sigmoid_gate).astype(BF16)
    spread = by_xor(double(jnp.concatenate([dgate, dup], axis=1), "dp"), bits)
    terms = backward(jnp.concatenate(spread, axis=0), w_gate, w_up)
    grads = scatter_rows(blocks_of(terms, len(image_all)), "tp")
    image_grad = grads[:image_dev].astype(BF16)
    text_part = grads[image_dev:].astype(BF16)
    live = lax.broadcasted_iota(jnp.int32, text_part.shape, 0) < text_count[0]
    text_grad = jnp.where(live, text_part, jnp.zeros_like(text_part))
    return (image_grad, text_grad)


def solution(mesh):
    placed = (
        P(("group", "tp"), "dp"),
        P(("group", "tp"), "dp"),
        P(("group", "tp"), "dp"),
        P(("group", "tp"), "dp"),
        P(("group", "tp"), None),
        P(("group", "tp")),
        P("dp", "tp"),
        P("dp", "tp"),
        P("tp", "dp"),
    )
    return jax.shard_map(
        per_device,
        mesh=mesh,
        in_specs=placed,
        out_specs=(P(("group", "tp"), "dp"), P(("group", "tp"), "dp")),
        check_vma=False,
    )
```

```python
import jax
import jax.numpy as jnp
from jax import lax
from jax.experimental import pallas as pl
from jax.experimental.pallas import tpu as pltpu
from jax.sharding import PartitionSpec as P


F32 = jnp.float32
BF16 = jnp.bfloat16
DIRECT = 4
LIMIT = 6 << 20
CHUNKS = 4
NT = (((1,), (1,)), ((), ()))


def in_vmem(value):
    return pltpu.with_memory_space_constraint(value, pltpu.VMEM)


def in_hbm(value):
    return pltpu.with_memory_space_constraint(value, pltpu.HBM)


def array(shape, dtype):
    return jax.ShapeDtypeStruct(shape, dtype)


def call(kernel, out_shape, values, kinds, flops=0, scratch=(), extra=0):
    memory = {"S": pltpu.SMEM, "V": pltpu.VMEM, "H": pltpu.HBM, "A": pl.ANY}
    values = [in_hbm(v) if kind == "H" else v for v, kind in zip(values, kinds)]
    nbytes = sum(v.size * v.dtype.itemsize for v in values)
    return pl.pallas_call(
        kernel,
        out_shape=out_shape,
        in_specs=[pl.BlockSpec(memory_space=memory[kind]) for kind in kinds],
        out_specs=jax.tree.map(lambda _: pl.BlockSpec(memory_space=pltpu.VMEM), out_shape),
        scratch_shapes=list(scratch),
        compiler_params=pltpu.CompilerParams(vmem_limit_bytes=LIMIT + extra),
        cost_estimate=pl.CostEstimate(flops=max(flops, nbytes), transcendentals=0, bytes_accessed=nbytes),
    )(*values)


def swapped(value, axis, bit):
    size = lax.axis_size(axis)
    return lax.ppermute(value, axis, [(i, i ^ bit) for i in range(size)])


def bits_of(size):
    return [1 << i for i in range(size.bit_length() - 1)]


def blocks_of(rows, count):
    return jnp.split(rows, count, axis=0)


def by_xor(blocks, bits):
    for n, bit in enumerate(bits_of(len(blocks))):
        flip = bits[n : n + 1, :1] != 0
        blocks = [jnp.where(flip, blocks[j ^ bit], blocks[j]) for j in range(len(blocks))]
    return blocks


def gather_rows(value, axis):
    size = lax.axis_size(axis)
    if size > DIRECT:
        return blocks_of(lax.all_gather(value, axis, axis=0, tiled=True), size)
    blocks = [value]
    for k in range(1, size):
        blocks.append(swapped(value, axis, k))
    return blocks


def scatter_rows(blocks, axis):
    size = lax.axis_size(axis)
    if size > DIRECT:
        joined = jnp.concatenate([b.astype(BF16) for b in blocks], axis=0)
        return lax.psum_scatter(joined, axis, scatter_dimension=0, tiled=True).astype(F32)
    total = blocks[0]
    sent = [b.astype(BF16) for b in blocks[1:]]
    for k in range(1, size):
        got = swapped(sent[k - 1], axis, k)
        total = total + got.astype(F32)
    return total


def copies_of(source, target, sems, count=CHUNKS):
    step = source.shape[0] // count
    rows = [pl.ds(i * step, step) for i in range(count)]
    return [pltpu.make_async_copy(source.at[r], target.at[r], sems.at[i]) for i, r in enumerate(rows)]


def loaded(weight, count, after):
    def kernel(w_ref, after_ref, out_ref, sems):
        copies = copies_of(w_ref.at[pl.ds(0, count)], out_ref, sems)
        for copy in copies:
            copy.start()
        for copy in copies:
            copy.wait()

    out = pltpu.VMEM((count, weight.shape[1]), weight.dtype)
    return call(kernel, out, (weight, after), "HA", int(4e9), [pltpu.SemaphoreType.DMA((CHUNKS,))])


def prepare(flags, image_slots, image_cot, text_rows, text_cot, destination, capacity):
    slots, feat = image_slots.shape
    two = slots == 2 * capacity
    text_dev = text_rows.shape[0]
    rows = destination.shape[0]
    kept = capacity if two else slots
    width = 2 * kept if two else kept

    def kernel(
        flags_ref, slots_ref, cot_ref, text_ref, text_cot_ref, target_hbm,
        own_ref, give_ref, text_out_ref, select_ref, bits_ref, target_ref, sems,
    ):
        pairs = [(target_hbm, target_ref)]
        for at, image, text in ((pl.ds(0, feat), slots_ref, text_ref), (pl.ds(feat, feat), cot_ref, text_cot_ref)):
            start = flags_ref[0] * capacity if two else 0
            pairs.append((image.at[pl.ds(start, kept)], own_ref.at[:, at]))
            pairs.append((text, text_out_ref.at[:, at]))
            if two:
                pairs.append((image.at[pl.ds(capacity - start, kept)], give_ref.at[:, at]))
        copies = [pltpu.make_async_copy(a, b, sems.at[i]) for i, (a, b) in enumerate(pairs)]
        for copy in copies:
            copy.start()
        row = lax.broadcasted_iota(jnp.int32, bits_ref.shape, 0)
        index = jnp.full(bits_ref.shape, flags_ref[1], jnp.int32)
        bits_ref[...] = lax.shift_right_logical(index, row) & 1
        if not two:
            give_ref[...] = jnp.zeros_like(give_ref)
        copies[0].wait()
        target = [target_ref[i] for i in range(rows)]
        first = flags_ref[0] if two else 0
        position = lax.broadcasted_iota(jnp.int32, (rows, width), 0)
        lane = lax.broadcasted_iota(jnp.int32, (rows, width), 1)
        column = jnp.zeros((rows, width), jnp.int32)
        for i in range(rows):
            rank = jnp.int32(0)
            for j in range(i):
                rank = rank + (target[j] == target[i]).astype(jnp.int32)
            slot = jnp.bitwise_xor(target[i], first) * capacity + rank
            column = jnp.where(position == i, slot, column)
        select_ref[...] = jnp.where(column == lane, 1.0, 0.0)
        for copy in copies[1:]:
            copy.wait()

    given = capacity if two else 8
    out = (
        array((kept, 2 * feat), BF16),
        array((given, 2 * feat), BF16),
        array((text_dev, 2 * feat), BF16),
        array((rows, width), F32),
        array((8, 128), jnp.int32),
    )
    values = (flags, image_slots, image_cot, text_rows, text_cot, destination)
    scratch = [pltpu.SMEM((rows,), jnp.int32), pltpu.SemaphoreType.DMA((7,))]
    return call(kernel, out, values, "SHHHHH", 0, scratch)


def pick(select, own, got, text, two):
    rows = select.shape[0]
    width = own.shape[1]

    def kernel(select_ref, own_ref, got_ref, text_ref, out_ref):
        select = select_ref[...].astype(BF16)
        if two:
            half = own_ref.shape[0]
            out = jnp.dot(select[:, :half], own_ref[...], preferred_element_type=F32)
            out = out + jnp.dot(select[:, half:], got_ref[...], preferred_element_type=F32)
        else:
            out = jnp.dot(select, own_ref[...], preferred_element_type=F32)
        out_ref[...] = jnp.concatenate([out.astype(BF16), text_ref[...]], axis=0)

    return call(kernel, array((rows + text.shape[0], width), BF16), (select, own, got, text), "VVVV")


def step_of(width):
    for step in (896, 512, 256):
        if width % step == 0:
            return step
    return 128


def split_store(out, keep_ref, give_ref, to, part):
    for i in range(out.shape[0] // part // 2):
        kept = out[2 * i * part : (2 * i + 1) * part]
        given = out[(2 * i + 1) * part : (2 * i + 2) * part]
        keep_ref[i * part : (i + 1) * part, to] = kept
        give_ref[i * part : (i + 1) * part, to] = given.astype(BF16)


def low_part(weight):
    return -(-weight.shape[0] // 1024) * 512


def forward_in(x, w_gate, w_up, parts):
    rows = x.shape[0]
    width = w_gate.shape[1]
    step = step_of(width)
    count = width // step

    def kernel(x_ref, gate_ref, up_hbm, keep_ref, give_ref, up_ref, up_sems):
        columns = [pl.ds(j * step, step) for j in range(count)]
        ups = [pltpu.make_async_copy(up_hbm.at[:, c], up_ref.at[:, c], up_sems.at[j]) for j, c in enumerate(columns)]
        for copy in ups:
            copy.start()
        for n, w_ref in enumerate((gate_ref, up_ref)):
            for j, at in enumerate(columns):
                if n == 1:
                    ups[j].wait()
                out = jnp.dot(x_ref[...], w_ref[:, at], preferred_element_type=F32)
                split_store(out, keep_ref, give_ref, pl.ds(n * width + j * step, step), rows // parts)

    out = (
        array((rows // 2, 2 * width), F32),
        array((rows // 2, 2 * width), BF16),
        pltpu.VMEM(w_up.shape, w_up.dtype),
    )
    values = (x, in_vmem(w_gate), w_up)
    scratch = [pltpu.SemaphoreType.DMA((count,))]
    return call(kernel, out, values, "VVH", 4 * rows * w_up.size, scratch)


def forward_back(x, weight, after, parts, first, width):
    rows = x.shape[0]
    step = 512 if width % 512 == 0 else 128
    count = width // step
    streamed = weight.shape[0] != width

    def kernel(x_ref, w_ref, after_ref, keep_ref, give_ref, *scratch):
        copies = []
        if streamed:
            copies = copies_of(w_ref.at[pl.ds(first, width)], *scratch, count)
            w_ref = scratch[0]
        for copy in copies:
            copy.start()
        for j in range(count):
            at = pl.ds(j * step, step)
            if streamed:
                copies[j].wait()
            out = lax.dot_general(x_ref[...], w_ref[at, :], NT, preferred_element_type=F32)
            split_store(out, keep_ref, give_ref, at, rows // parts)

    out = (array((rows // 2, width), F32), array((rows // 2, width), BF16))
    scratch = []
    extra = 0
    if streamed:
        scratch = [pltpu.VMEM((width, weight.shape[1]), weight.dtype), pltpu.SemaphoreType.DMA((count,))]
        extra = width * weight.shape[1] * 2
    values = (x, weight if streamed else in_vmem(weight), after)
    flops = 2 * rows * width * weight.shape[1]
    return call(kernel, out, values, "VHA" if streamed else "VVA", flops, scratch, extra)


def halve_first(give, keep, axis):
    half = lax.axis_size(axis) // 2
    got = blocks_of(swapped(give, axis, 1), half)
    return [a + b.astype(F32) for a, b in zip(blocks_of(keep, half), got)]


def sent_rows(blocks):
    return jnp.concatenate([b.astype(BF16) for b in blocks[1::2]], axis=0)


def halve_rest(blocks, axis, sent):
    for bit in bits_of(lax.axis_size(axis))[1:]:
        got = blocks_of(swapped(sent, axis, bit), len(blocks) // 2)
        blocks = [a + b.astype(F32) for a, b in zip(blocks[0::2], got)]
        sent = sent_rows(blocks) if len(blocks) > 1 else None
    return blocks[0]


def double(value, axis):
    pieces = [value]
    for bit in reversed(bits_of(lax.axis_size(axis))):
        got = blocks_of(swapped(jnp.concatenate(pieces, axis=0), axis, bit), len(pieces))
        pieces = [b for pair in zip(pieces, got) for b in pair]
    return pieces


def backward(x, weight, added=None):
    rows = x.shape[0]
    feat = weight.shape[0]
    step = 512 if feat % 512 == 0 else 128
    more = 0 if added is None else 1

    def kernel(x_ref, w_ref, *refs):
        out_ref = refs[more]
        for j in range(feat // step):
            at = pl.ds(j * step, step)
            out = lax.dot_general(x_ref[...], w_ref[at, :], NT, preferred_element_type=F32)
            out_ref[:, at] = out + refs[0][:, at] if more else out

    values = (x, in_vmem(weight), *([added] * more))
    return call(kernel, array((rows, feat), F32), values, "VV" + "V" * more, 2 * rows * weight.size)


def per_device(
    image_slots, image_cot, text_rows, text_cot, destination, text_count, w_gate, w_up, w_down
):
    groups = lax.axis_size("group")
    parts = lax.axis_size("dp")
    capacity = image_slots.shape[0] // groups
    image_dev = destination.shape[0]
    feat, hidden = w_gate.shape
    two = groups == 2
    flags = jnp.stack([lax.axis_index("group"), lax.axis_index("dp")]).astype(jnp.int32)
    target = destination.reshape(image_dev)
    own, give, text, select, bits = prepare(flags, image_slots, image_cot, text_rows, text_cot, target, capacity)
    if two:
        got = swapped(give, "group", 1)
    else:
        own = lax.all_to_all(own, "group", split_axis=0, concat_axis=0, tiled=True)
        got = give
    low = low_part(w_down)
    picked = pick(select, own, got, text, two)
    gathered = gather_rows(picked, "tp")
    w_gate = loaded(w_gate, w_gate.shape[0], picked)
    down_low = loaded(w_down, low, picked)
    rows = jnp.concatenate(gathered, axis=0)
    rows = jnp.concatenate(by_xor(blocks_of(rows, parts), bits), axis=0)

    keep, give, w_up = forward_in(rows[:, :feat], w_gate, w_up, parts)
    both = halve_first(give, keep, "dp")
    cot = rows[:, feat:]
    sent = sent_rows(both)
    keep_low, give_low = forward_back(cot, down_low, give, parts, 0, low)
    keep_high, give_high = forward_back(cot, w_down, sent, parts, low, hidden - low)
    both = halve_rest(both, "dp", sent)
    keep = jnp.concatenate([keep_low, keep_high], axis=1)
    give = jnp.concatenate([give_low, give_high], axis=1)
    back = halve_first(give, keep, "dp")
    back = halve_rest(back, "dp", sent_rows(back))

    gate = both[:, :hidden]
    up = both[:, hidden:]
    sigmoid_gate = jax.nn.sigmoid(gate)
    dgate = (back * up * sigmoid_gate * (1.0 + gate * (1.0 - sigmoid_gate))).astype(BF16)
    dup = (back * gate * sigmoid_gate).astype(BF16)
    spread_gate = by_xor(double(dgate, "dp"), bits)
    spread_up = by_xor(double(dup, "dp"), bits)
    terms = backward(jnp.concatenate(spread_gate, axis=0), w_gate)
    terms = backward(jnp.concatenate(spread_up, axis=0), w_up, terms)
    grads = scatter_rows(blocks_of(terms, len(gathered)), "tp")
    image_grad = grads[:image_dev].astype(BF16)
    text_part = grads[image_dev:].astype(BF16)
    live = lax.broadcasted_iota(jnp.int32, text_part.shape, 0) < text_count[0]
    text_grad = jnp.where(live, text_part, jnp.zeros_like(text_part))
    return (image_grad, text_grad)


def solution(mesh):
    placed = (
        P(("group", "tp"), "dp"),
        P(("group", "tp"), "dp"),
        P(("group", "tp"), "dp"),
        P(("group", "tp"), "dp"),
        P(("group", "tp"), None),
        P(("group", "tp")),
        P("dp", "tp"),
        P("dp", "tp"),
        P("tp", "dp"),
    )
    return jax.shard_map(
        per_device,
        mesh=mesh,
        in_specs=placed,
        out_specs=(P(("group", "tp"), "dp"), P(("group", "tp"), "dp")),
        check_vma=False,
    )
```

```python
import jax
import jax.numpy as jnp
from jax import lax
from jax.experimental import pallas as pl
from jax.experimental.pallas import tpu as pltpu
from jax.sharding import PartitionSpec as P


F32 = jnp.float32
BF16 = jnp.bfloat16
DIRECT = 4
LIMIT = 6 << 20
CHUNKS = 4
NT = (((1,), (1,)), ((), ()))


def in_vmem(value):
    return pltpu.with_memory_space_constraint(value, pltpu.VMEM)


def in_hbm(value):
    return pltpu.with_memory_space_constraint(value, pltpu.HBM)


def array(shape, dtype):
    return jax.ShapeDtypeStruct(shape, dtype)


def call(kernel, out_shape, values, kinds, flops=0, scratch=(), extra=0):
    memory = {"S": pltpu.SMEM, "V": pltpu.VMEM, "H": pltpu.HBM, "A": pl.ANY}
    values = [in_hbm(v) if kind == "H" else v for v, kind in zip(values, kinds)]
    nbytes = sum(v.size * v.dtype.itemsize for v in values)
    return pl.pallas_call(
        kernel,
        out_shape=out_shape,
        in_specs=[pl.BlockSpec(memory_space=memory[kind]) for kind in kinds],
        out_specs=jax.tree.map(lambda _: pl.BlockSpec(memory_space=pltpu.VMEM), out_shape),
        scratch_shapes=list(scratch),
        compiler_params=pltpu.CompilerParams(vmem_limit_bytes=LIMIT + extra),
        cost_estimate=pl.CostEstimate(flops=max(flops, nbytes), transcendentals=0, bytes_accessed=nbytes),
    )(*values)


def swapped(value, axis, bit):
    size = lax.axis_size(axis)
    return lax.ppermute(value, axis, [(i, i ^ bit) for i in range(size)])


def bits_of(size):
    return [1 << i for i in range(size.bit_length() - 1)]


def blocks_of(rows, count):
    return jnp.split(rows, count, axis=0)


def by_xor(blocks, bits):
    for n, bit in enumerate(bits_of(len(blocks))):
        flip = bits[n : n + 1, :1] != 0
        blocks = [jnp.where(flip, blocks[j ^ bit], blocks[j]) for j in range(len(blocks))]
    return blocks


def gather_rows(value, axis):
    size = lax.axis_size(axis)
    if size > DIRECT:
        return blocks_of(lax.all_gather(value, axis, axis=0, tiled=True), size)
    blocks = [value]
    for k in range(1, size):
        blocks.append(swapped(value, axis, k))
    return blocks


def scatter_rows(blocks, axis):
    size = lax.axis_size(axis)
    if size > DIRECT:
        joined = jnp.concatenate([b.astype(BF16) for b in blocks], axis=0)
        return lax.psum_scatter(joined, axis, scatter_dimension=0, tiled=True).astype(F32)
    total = blocks[0]
    sent = [b.astype(BF16) for b in blocks[1:]]
    for k in range(1, size):
        got = swapped(sent[k - 1], axis, k)
        total = total + got.astype(F32)
    return total


def copies_of(source, target, sems, count=CHUNKS):
    step = source.shape[0] // count
    rows = [pl.ds(i * step, step) for i in range(count)]
    return [pltpu.make_async_copy(source.at[r], target.at[r], sems.at[i]) for i, r in enumerate(rows)]


def loaded(weight, count, after):
    def kernel(w_ref, after_ref, out_ref, sems):
        copies = copies_of(w_ref.at[pl.ds(0, count)], out_ref, sems)
        for copy in copies:
            copy.start()
        for copy in copies:
            copy.wait()

    out = pltpu.VMEM((count, weight.shape[1]), weight.dtype)
    return call(kernel, out, (weight, after), "HA", int(4e9), [pltpu.SemaphoreType.DMA((CHUNKS,))])


def prepare(image_slots, image_cot, text_rows, text_cot, destination, capacity):
    slots, feat = image_slots.shape
    two = slots == 2 * capacity
    text_dev = text_rows.shape[0]
    rows = destination.shape[0]
    kept = capacity if two else slots
    width = 2 * kept if two else kept

    def kernel(
        slots_ref, cot_ref, text_ref, text_cot_ref, target_hbm,
        own_ref, give_ref, text_out_ref, select_ref, bits_ref, target_ref, sems,
    ):
        group = lax.axis_index("group")
        pairs = [(target_hbm, target_ref)]
        for at, image, text in ((pl.ds(0, feat), slots_ref, text_ref), (pl.ds(feat, feat), cot_ref, text_cot_ref)):
            start = group * capacity if two else 0
            pairs.append((image.at[pl.ds(start, kept)], own_ref.at[:, at]))
            pairs.append((text, text_out_ref.at[:, at]))
            if two:
                pairs.append((image.at[pl.ds(capacity - start, kept)], give_ref.at[:, at]))
        copies = [pltpu.make_async_copy(a, b, sems.at[i]) for i, (a, b) in enumerate(pairs)]
        for copy in copies:
            copy.start()
        row = lax.broadcasted_iota(jnp.int32, bits_ref.shape, 0)
        index = jnp.full(bits_ref.shape, lax.axis_index("dp"), jnp.int32)
        bits_ref[...] = lax.shift_right_logical(index, row) & 1
        if not two:
            give_ref[...] = jnp.zeros_like(give_ref)
        copies[0].wait()
        target = [target_ref[i] for i in range(rows)]
        first = group if two else 0
        position = lax.broadcasted_iota(jnp.int32, (rows, width), 0)
        lane = lax.broadcasted_iota(jnp.int32, (rows, width), 1)
        column = jnp.zeros((rows, width), jnp.int32)
        for i in range(rows):
            rank = jnp.int32(0)
            for j in range(i):
                rank = rank + (target[j] == target[i]).astype(jnp.int32)
            slot = jnp.bitwise_xor(target[i], first) * capacity + rank
            column = jnp.where(position == i, slot, column)
        select_ref[...] = jnp.where(column == lane, 1.0, 0.0)
        for copy in copies[1:]:
            copy.wait()

    given = capacity if two else 8
    out = (
        array((kept, 2 * feat), BF16),
        array((given, 2 * feat), BF16),
        array((text_dev, 2 * feat), BF16),
        array((rows, width), F32),
        array((8, 128), jnp.int32),
    )
    values = (image_slots, image_cot, text_rows, text_cot, destination)
    scratch = [pltpu.SMEM((rows,), jnp.int32), pltpu.SemaphoreType.DMA((7,))]
    return call(kernel, out, values, "HHHHH", 0, scratch)


def pick(select, own, got, text, two):
    rows = select.shape[0]
    width = own.shape[1]

    def kernel(select_ref, own_ref, got_ref, text_ref, out_ref):
        select = select_ref[...].astype(BF16)
        if two:
            half = own_ref.shape[0]
            out = jnp.dot(select[:, :half], own_ref[...], preferred_element_type=F32)
            out = out + jnp.dot(select[:, half:], got_ref[...], preferred_element_type=F32)
        else:
            out = jnp.dot(select, own_ref[...], preferred_element_type=F32)
        out_ref[...] = jnp.concatenate([out.astype(BF16), text_ref[...]], axis=0)

    return call(kernel, array((rows + text.shape[0], width), BF16), (select, own, got, text), "VVVV")


def step_of(width):
    for step in (896, 512, 256):
        if width % step == 0:
            return step
    return 128


def split_store(out, keep_ref, give_ref, to, part):
    for i in range(out.shape[0] // part // 2):
        kept = out[2 * i * part : (2 * i + 1) * part]
        given = out[(2 * i + 1) * part : (2 * i + 2) * part]
        keep_ref[i * part : (i + 1) * part, to] = kept
        give_ref[i * part : (i + 1) * part, to] = given.astype(BF16)


def low_part(weight):
    return -(-weight.shape[0] // 1024) * 512


def forward_in(x, w_gate, w_up, parts):
    rows = x.shape[0]
    width = w_gate.shape[1]
    step = step_of(width)
    count = width // step

    def kernel(x_ref, gate_ref, up_hbm, keep_ref, give_ref, up_ref, up_sems):
        columns = [pl.ds(j * step, step) for j in range(count)]
        ups = [pltpu.make_async_copy(up_hbm.at[:, c], up_ref.at[:, c], up_sems.at[j]) for j, c in enumerate(columns)]
        for copy in ups:
            copy.start()
        for n, w_ref in enumerate((gate_ref, up_ref)):
            for j, at in enumerate(columns):
                if n == 1:
                    ups[j].wait()
                out = jnp.dot(x_ref[...], w_ref[:, at], preferred_element_type=F32)
                split_store(out, keep_ref, give_ref, pl.ds(n * width + j * step, step), rows // parts)

    out = (
        array((rows // 2, 2 * width), F32),
        array((rows // 2, 2 * width), BF16),
        pltpu.VMEM(w_up.shape, w_up.dtype),
    )
    values = (x, in_vmem(w_gate), w_up)
    scratch = [pltpu.SemaphoreType.DMA((count,))]
    return call(kernel, out, values, "VVH", 4 * rows * w_up.size, scratch)


def forward_back(x, weight, after, parts, first, width):
    rows = x.shape[0]
    streamed = weight.shape[0] != width
    step = 512 if streamed else 256
    step = step if width % step == 0 else 128
    count = width // step

    def kernel(x_ref, w_ref, after_ref, keep_ref, give_ref, *scratch):
        copies = []
        if streamed:
            copies = copies_of(w_ref.at[pl.ds(first, width)], *scratch, count)
            w_ref = scratch[0]
        for copy in copies:
            copy.start()
        for j in range(count):
            at = pl.ds(j * step, step)
            if streamed:
                copies[j].wait()
            if streamed:
                out = lax.dot_general(x_ref[...], w_ref[at, :], NT, preferred_element_type=F32)
            else:
                out = lax.dot_general(w_ref[at, :], x_ref[...], NT, preferred_element_type=F32).T
            split_store(out, keep_ref, give_ref, at, rows // parts)

    out = (array((rows // 2, width), F32), array((rows // 2, width), BF16))
    scratch = []
    extra = 0
    if streamed:
        scratch = [pltpu.VMEM((width, weight.shape[1]), weight.dtype), pltpu.SemaphoreType.DMA((count,))]
        extra = width * weight.shape[1] * 2
    values = (x, weight if streamed else in_vmem(weight), after)
    flops = 2 * rows * width * weight.shape[1]
    return call(kernel, out, values, "VHA" if streamed else "VVA", flops, scratch, extra)


def halve_first(give, keep, axis):
    half = lax.axis_size(axis) // 2
    got = blocks_of(swapped(give, axis, 1), half)
    return [a + b.astype(F32) for a, b in zip(blocks_of(keep, half), got)]


def sent_rows(blocks):
    return jnp.concatenate([b.astype(BF16) for b in blocks[1::2]], axis=0)


def halve_rest(blocks, axis, sent):
    for bit in bits_of(lax.axis_size(axis))[1:]:
        got = blocks_of(swapped(sent, axis, bit), len(blocks) // 2)
        blocks = [a + b.astype(F32) for a, b in zip(blocks[0::2], got)]
        sent = sent_rows(blocks) if len(blocks) > 1 else None
    return blocks[0]


def double(value, axis):
    pieces = [value]
    for bit in reversed(bits_of(lax.axis_size(axis))):
        got = blocks_of(swapped(jnp.concatenate(pieces, axis=0), axis, bit), len(pieces))
        pieces = [b for pair in zip(pieces, got) for b in pair]
    return pieces


def backward(x, weights, added=None):
    rows = x.shape[0]
    feat = weights[0].shape[0]
    step = 256
    count = len(weights)
    more = 0 if added is None else 1

    def kernel(x_ref, *refs):
        out_ref = refs[count + more]
        for j in range(feat // step):
            at = pl.ds(j * step, step)
            start = 0
            out = None
            for w_ref in refs[:count]:
                columns = pl.ds(start, w_ref.shape[1])
                term = lax.dot_general(w_ref[at, :], x_ref[:, columns], NT, preferred_element_type=F32)
                out = term if out is None else out + term
                start += w_ref.shape[1]
            out = out.T
            out_ref[:, at] = out + refs[count][:, at] if more else out

    values = (x, *[in_vmem(w) for w in weights], *([added] * more))
    flops = 2 * rows * feat * x.shape[1]
    return call(kernel, array((rows, feat), F32), values, "V" * len(values), flops)


def per_device(
    image_slots, image_cot, text_rows, text_cot, destination, text_count, w_gate, w_up, w_down
):
    groups = lax.axis_size("group")
    parts = lax.axis_size("dp")
    capacity = image_slots.shape[0] // groups
    image_dev = destination.shape[0]
    feat, hidden = w_gate.shape
    two = groups == 2
    target = destination.reshape(image_dev)
    own, give, text, select, bits = prepare(image_slots, image_cot, text_rows, text_cot, target, capacity)
    if two:
        got = swapped(give, "group", 1)
    else:
        own = lax.all_to_all(own, "group", split_axis=0, concat_axis=0, tiled=True)
        got = give
    low = low_part(w_down)
    picked = pick(select, own, got, text, two)
    gathered = gather_rows(picked, "tp")
    w_gate = loaded(w_gate, w_gate.shape[0], picked)
    down_low = loaded(w_down, low, picked)
    rows = jnp.concatenate(gathered, axis=0)
    rows = jnp.concatenate(by_xor(blocks_of(rows, parts), bits), axis=0)

    keep, give, w_up = forward_in(rows[:, :feat], w_gate, w_up, parts)
    both = halve_first(give, keep, "dp")
    cot = rows[:, feat:]
    sent = sent_rows(both)
    keep_low, give_low = forward_back(cot, down_low, give, parts, 0, low)
    keep_high, give_high = forward_back(cot, w_down, sent, parts, low, hidden - low)
    both = halve_rest(both, "dp", sent)
    back_low = halve_first(give_low, keep_low, "dp")
    back_high = halve_first(give_high, keep_high, "dp")
    back_low = halve_rest(back_low, "dp", sent_rows(back_low))
    sent = sent_rows(back_high)
    back_high = halve_rest(back_high, "dp", sent)
    back = jnp.concatenate([back_low, back_high], axis=1)

    gate = both[:, :hidden]
    up = both[:, hidden:]
    sigmoid_gate = jax.nn.sigmoid(gate)
    dgate = (back * up * sigmoid_gate * (1.0 + gate * (1.0 - sigmoid_gate))).astype(BF16)
    dup = (back * gate * sigmoid_gate).astype(BF16)
    spread_gate = by_xor(double(dgate, "dp"), bits)
    spread_up = by_xor(double(dup, "dp"), bits)
    terms = backward(jnp.concatenate(spread_gate, axis=0), (w_gate,))
    terms = backward(jnp.concatenate(spread_up, axis=0), (w_up,), terms)
    grads = scatter_rows(blocks_of(terms, len(gathered)), "tp")
    image_grad = grads[:image_dev].astype(BF16)
    text_part = grads[image_dev:].astype(BF16)
    live = lax.broadcasted_iota(jnp.int32, text_part.shape, 0) < text_count[0]
    text_grad = jnp.where(live, text_part, jnp.zeros_like(text_part))
    return (image_grad, text_grad)


def solution(mesh):
    placed = (
        P(("group", "tp"), "dp"),
        P(("group", "tp"), "dp"),
        P(("group", "tp"), "dp"),
        P(("group", "tp"), "dp"),
        P(("group", "tp"), None),
        P(("group", "tp")),
        P("dp", "tp"),
        P("dp", "tp"),
        P("tp", "dp"),
    )
    return jax.shard_map(
        per_device,
        mesh=mesh,
        in_specs=placed,
        out_specs=(P(("group", "tp"), "dp"), P(("group", "tp"), "dp")),
        check_vma=False,
    )
```

```python
import jax
import jax.numpy as jnp
from jax import lax
from jax.experimental import pallas as pl
from jax.experimental.pallas import tpu as pltpu
from jax.sharding import PartitionSpec as P


F32 = jnp.float32
BF16 = jnp.bfloat16
DIRECT = 4
LIMIT = 6 << 20
CHUNKS = 4
NT = (((1,), (1,)), ((), ()))


def in_vmem(value):
    return pltpu.with_memory_space_constraint(value, pltpu.VMEM)


def in_hbm(value):
    return pltpu.with_memory_space_constraint(value, pltpu.HBM)


def array(shape, dtype):
    return jax.ShapeDtypeStruct(shape, dtype)


def call(kernel, out_shape, values, kinds, flops=0, scratch=(), extra=0):
    memory = {"S": pltpu.SMEM, "V": pltpu.VMEM, "H": pltpu.HBM, "A": pl.ANY}
    values = [in_hbm(v) if kind == "H" else v for v, kind in zip(values, kinds)]
    nbytes = sum(v.size * v.dtype.itemsize for v in values)
    return pl.pallas_call(
        kernel,
        out_shape=out_shape,
        in_specs=[pl.BlockSpec(memory_space=memory[kind]) for kind in kinds],
        out_specs=jax.tree.map(lambda _: pl.BlockSpec(memory_space=pltpu.VMEM), out_shape),
        scratch_shapes=list(scratch),
        compiler_params=pltpu.CompilerParams(vmem_limit_bytes=LIMIT + extra),
        cost_estimate=pl.CostEstimate(flops=max(flops, nbytes), transcendentals=0, bytes_accessed=nbytes),
    )(*values)


def swapped(value, axis, bit):
    size = lax.axis_size(axis)
    return lax.ppermute(value, axis, [(i, i ^ bit) for i in range(size)])


def bits_of(size):
    return [1 << i for i in range(size.bit_length() - 1)]


def blocks_of(rows, count):
    return jnp.split(rows, count, axis=0)


def by_xor(blocks, bits):
    for n, bit in enumerate(bits_of(len(blocks))):
        flip = bits[n : n + 1, :1] != 0
        blocks = [jnp.where(flip, blocks[j ^ bit], blocks[j]) for j in range(len(blocks))]
    return blocks


def gather_rows(value, axis):
    size = lax.axis_size(axis)
    if size > DIRECT:
        return blocks_of(lax.all_gather(value, axis, axis=0, tiled=True), size)
    blocks = [value]
    for k in range(1, size):
        blocks.append(swapped(value, axis, k))
    return blocks


def scatter_rows(blocks, axis):
    size = lax.axis_size(axis)
    if size > DIRECT:
        joined = jnp.concatenate([b.astype(BF16) for b in blocks], axis=0)
        return lax.psum_scatter(joined, axis, scatter_dimension=0, tiled=True).astype(F32)
    total = blocks[0]
    sent = [b.astype(BF16) for b in blocks[1:]]
    for k in range(1, size):
        got = swapped(sent[k - 1], axis, k)
        total = total + got.astype(F32)
    return total


def copies_of(source, target, sems, count=CHUNKS):
    step = source.shape[0] // count
    rows = [pl.ds(i * step, step) for i in range(count)]
    return [pltpu.make_async_copy(source.at[r], target.at[r], sems.at[i]) for i, r in enumerate(rows)]


def loaded(weight, count, after):
    def kernel(w_ref, after_ref, out_ref, sems):
        copies = copies_of(w_ref.at[pl.ds(0, count)], out_ref, sems)
        for copy in copies:
            copy.start()
        for copy in copies:
            copy.wait()

    out = pltpu.VMEM((count, weight.shape[1]), weight.dtype)
    return call(kernel, out, (weight, after), "HA", int(4e9), [pltpu.SemaphoreType.DMA((CHUNKS,))])


def prepare(image_slots, image_cot, text_rows, text_cot, destination, capacity):
    slots, feat = image_slots.shape
    two = slots == 2 * capacity
    text_dev = text_rows.shape[0]
    rows = destination.shape[0]
    kept = capacity if two else slots
    width = 2 * kept if two else kept

    def kernel(
        slots_ref, cot_ref, text_ref, text_cot_ref, target_hbm,
        own_ref, give_ref, text_out_ref, select_ref, bits_ref, target_ref, sems,
    ):
        group = lax.axis_index("group")
        pairs = [(target_hbm, target_ref)]
        for at, image, text in ((pl.ds(0, feat), slots_ref, text_ref), (pl.ds(feat, feat), cot_ref, text_cot_ref)):
            start = group * capacity if two else 0
            pairs.append((image.at[pl.ds(start, kept)], own_ref.at[:, at]))
            pairs.append((text, text_out_ref.at[:, at]))
            if two:
                pairs.append((image.at[pl.ds(capacity - start, kept)], give_ref.at[:, at]))
        copies = [pltpu.make_async_copy(a, b, sems.at[i]) for i, (a, b) in enumerate(pairs)]
        for copy in copies:
            copy.start()
        row = lax.broadcasted_iota(jnp.int32, bits_ref.shape, 0)
        index = jnp.full(bits_ref.shape, lax.axis_index("dp"), jnp.int32)
        bits_ref[...] = lax.shift_right_logical(index, row) & 1
        if not two:
            give_ref[...] = jnp.zeros_like(give_ref)
        copies[0].wait()
        target = [target_ref[i] for i in range(rows)]
        first = group if two else 0
        position = lax.broadcasted_iota(jnp.int32, (rows, width), 0)
        lane = lax.broadcasted_iota(jnp.int32, (rows, width), 1)
        column = jnp.zeros((rows, width), jnp.int32)
        for i in range(rows):
            rank = jnp.int32(0)
            for j in range(i):
                rank = rank + (target[j] == target[i]).astype(jnp.int32)
            slot = jnp.bitwise_xor(target[i], first) * capacity + rank
            column = jnp.where(position == i, slot, column)
        select_ref[...] = jnp.where(column == lane, 1.0, 0.0)
        for copy in copies[1:]:
            copy.wait()

    given = capacity if two else 8
    out = (
        array((kept, 2 * feat), BF16),
        array((given, 2 * feat), BF16),
        array((text_dev, 2 * feat), BF16),
        array((rows, width), F32),
        array((8, 128), jnp.int32),
    )
    values = (image_slots, image_cot, text_rows, text_cot, destination)
    scratch = [pltpu.SMEM((rows,), jnp.int32), pltpu.SemaphoreType.DMA((7,))]
    return call(kernel, out, values, "HHHHH", 0, scratch)


def pick(select, own, got, text, two):
    rows = select.shape[0]
    width = own.shape[1]

    def kernel(select_ref, own_ref, got_ref, text_ref, out_ref):
        select = select_ref[...].astype(BF16)
        if two:
            half = own_ref.shape[0]
            out = jnp.dot(select[:, :half], own_ref[...], preferred_element_type=F32)
            out = out + jnp.dot(select[:, half:], got_ref[...], preferred_element_type=F32)
        else:
            out = jnp.dot(select, own_ref[...], preferred_element_type=F32)
        out_ref[...] = jnp.concatenate([out.astype(BF16), text_ref[...]], axis=0)

    return call(kernel, array((rows + text.shape[0], width), BF16), (select, own, got, text), "VVVV")


def step_of(width):
    for step in (896, 512, 256):
        if width % step == 0:
            return step
    return 128


def split_store(out, keep_ref, give_ref, to, part):
    for i in range(out.shape[0] // part // 2):
        kept = out[2 * i * part : (2 * i + 1) * part]
        given = out[(2 * i + 1) * part : (2 * i + 2) * part]
        keep_ref[i * part : (i + 1) * part, to] = kept
        give_ref[i * part : (i + 1) * part, to] = given.astype(BF16)


def low_part(weight):
    return -(-weight.shape[0] // 1024) * 512


def forward_in(x, w_gate, w_up, parts):
    rows = x.shape[0]
    width = w_gate.shape[1]
    step = step_of(width)
    count = width // step

    def kernel(x_ref, gate_ref, up_hbm, keep_ref, give_ref, up_ref, up_sems):
        columns = [pl.ds(j * step, step) for j in range(count)]
        ups = [pltpu.make_async_copy(up_hbm.at[:, c], up_ref.at[:, c], up_sems.at[j]) for j, c in enumerate(columns)]
        for copy in ups:
            copy.start()
        for n, w_ref in enumerate((gate_ref, up_ref)):
            for j, at in enumerate(columns):
                if n == 1:
                    ups[j].wait()
                out = jnp.dot(x_ref[...], w_ref[:, at], preferred_element_type=F32)
                split_store(out, keep_ref, give_ref, pl.ds(n * width + j * step, step), rows // parts)

    out = (
        array((rows // 2, 2 * width), F32),
        array((rows // 2, 2 * width), BF16),
        pltpu.VMEM(w_up.shape, w_up.dtype),
    )
    values = (x, in_vmem(w_gate), w_up)
    scratch = [pltpu.SemaphoreType.DMA((count,))]
    return call(kernel, out, values, "VVH", 4 * rows * w_up.size, scratch)


def forward_back(x, low, weight, after, parts, first, width):
    rows = x.shape[0]
    held = min(low.shape[0] - first, width)
    rest = width - held
    step = 512 if rest % 512 == 0 else 128
    count = rest // step

    def kernel(x_ref, low_ref, w_ref, after_ref, keep_ref, give_ref, *scratch):
        copies = []
        if rest:
            copies = copies_of(w_ref.at[pl.ds(first + held, rest)], *scratch, count)
        for copy in copies:
            copy.start()
        size = 256 if held % 256 == 0 else 128
        for j in range(held // size):
            at = pl.ds(j * size, size)
            out = lax.dot_general(low_ref[pl.ds(first + j * size, size), :], x_ref[...], NT, preferred_element_type=F32)
            split_store(out.T, keep_ref, give_ref, at, rows // parts)
        for j, copy in enumerate(copies):
            copy.wait()
            at = pl.ds(j * step, step)
            out = lax.dot_general(x_ref[...], scratch[0][at, :], NT, preferred_element_type=F32)
            split_store(out, keep_ref, give_ref, pl.ds(held + j * step, step), rows // parts)

    out = (array((rows // 2, width), F32), array((rows // 2, width), BF16))
    scratch = []
    if rest:
        scratch = [pltpu.VMEM((rest, weight.shape[1]), weight.dtype), pltpu.SemaphoreType.DMA((count,))]
    values = (x, in_vmem(low), weight, after)
    flops = 2 * rows * width * weight.shape[1]
    extra = 2 * rest * weight.shape[1]
    return call(kernel, out, values, "VVHA", flops, scratch, extra)


def halve_first(give, keep, axis):
    half = lax.axis_size(axis) // 2
    got = blocks_of(swapped(give, axis, 1), half)
    return [a + b.astype(F32) for a, b in zip(blocks_of(keep, half), got)]


def sent_rows(blocks):
    return jnp.concatenate([b.astype(BF16) for b in blocks[1::2]], axis=0)


def halve_rest(blocks, axis, sent):
    for bit in bits_of(lax.axis_size(axis))[1:]:
        got = blocks_of(swapped(sent, axis, bit), len(blocks) // 2)
        blocks = [a + b.astype(F32) for a, b in zip(blocks[0::2], got)]
        sent = sent_rows(blocks) if len(blocks) > 1 else None
    return blocks[0]


def double(value, axis):
    pieces = [value]
    for bit in reversed(bits_of(lax.axis_size(axis))):
        got = blocks_of(swapped(jnp.concatenate(pieces, axis=0), axis, bit), len(pieces))
        pieces = [b for pair in zip(pieces, got) for b in pair]
    return pieces


def backward(x, weights, added=None):
    rows = x.shape[0]
    feat = weights[0].shape[0]
    step = 256
    count = len(weights)
    more = 0 if added is None else 1

    def kernel(x_ref, *refs):
        out_ref = refs[count + more]
        for j in range(feat // step):
            at = pl.ds(j * step, step)
            start = 0
            out = None
            for w_ref in refs[:count]:
                columns = pl.ds(start, w_ref.shape[1])
                term = lax.dot_general(w_ref[at, :], x_ref[:, columns], NT, preferred_element_type=F32)
                out = term if out is None else out + term
                start += w_ref.shape[1]
            out = out.T
            out_ref[:, at] = out + refs[count][:, at] if more else out

    values = (x, *[in_vmem(w) for w in weights], *([added] * more))
    flops = 2 * rows * feat * x.shape[1]
    return call(kernel, array((rows, feat), F32), values, "V" * len(values), flops)


def per_device(
    image_slots, image_cot, text_rows, text_cot, destination, text_count, w_gate, w_up, w_down
):
    groups = lax.axis_size("group")
    parts = lax.axis_size("dp")
    capacity = image_slots.shape[0] // groups
    image_dev = destination.shape[0]
    feat, hidden = w_gate.shape
    two = groups == 2
    target = destination.reshape(image_dev)
    own, give, text, select, bits = prepare(image_slots, image_cot, text_rows, text_cot, target, capacity)
    if two:
        got = swapped(give, "group", 1)
    else:
        own = lax.all_to_all(own, "group", split_axis=0, concat_axis=0, tiled=True)
        got = give
    low = low_part(w_down)
    picked = pick(select, own, got, text, two)
    gathered = gather_rows(picked, "tp")
    w_gate = loaded(w_gate, w_gate.shape[0], picked)
    down_low = loaded(w_down, low, picked)
    rows = jnp.concatenate(gathered, axis=0)
    rows = jnp.concatenate(by_xor(blocks_of(rows, parts), bits), axis=0)

    keep, give, w_up = forward_in(rows[:, :feat], w_gate, w_up, parts)
    both = halve_first(give, keep, "dp")
    cot = rows[:, feat:]
    sent = sent_rows(both)
    split = max(low - 512, 256)
    keep_low, give_low = forward_back(cot, down_low, w_down, give, parts, 0, split)
    keep_high, give_high = forward_back(cot, down_low, w_down, sent, parts, split, hidden - split)
    both = halve_rest(both, "dp", sent)
    back_low = halve_first(give_low, keep_low, "dp")
    back_high = halve_first(give_high, keep_high, "dp")
    sent = sent_rows(back_low)
    back_low = halve_rest(back_low, "dp", sent)
    sent = sent_rows(back_high)
    back_high = halve_rest(back_high, "dp", sent)
    back = jnp.concatenate([back_low, back_high], axis=1)

    gate = both[:, :hidden]
    up = both[:, hidden:]
    sigmoid_gate = jax.nn.sigmoid(gate)
    dgate = (back * up * sigmoid_gate * (1.0 + gate * (1.0 - sigmoid_gate))).astype(BF16)
    dup = (back * gate * sigmoid_gate).astype(BF16)
    spread_gate = by_xor(double(dgate, "dp"), bits)
    spread_up = by_xor(double(dup, "dp"), bits)
    terms = backward(jnp.concatenate(spread_gate, axis=0), (w_gate,))
    terms = backward(jnp.concatenate(spread_up, axis=0), (w_up,), terms)
    grads = scatter_rows(blocks_of(terms, len(gathered)), "tp")
    image_grad = grads[:image_dev].astype(BF16)
    text_part = grads[image_dev:].astype(BF16)
    live = lax.broadcasted_iota(jnp.int32, text_part.shape, 0) < text_count[0]
    text_grad = jnp.where(live, text_part, jnp.zeros_like(text_part))
    return (image_grad, text_grad)


def solution(mesh):
    placed = (
        P(("group", "tp"), "dp"),
        P(("group", "tp"), "dp"),
        P(("group", "tp"), "dp"),
        P(("group", "tp"), "dp"),
        P(("group", "tp"), None),
        P(("group", "tp")),
        P("dp", "tp"),
        P("dp", "tp"),
        P("tp", "dp"),
    )
    return jax.shard_map(
        per_device,
        mesh=mesh,
        in_specs=placed,
        out_specs=(P(("group", "tp"), "dp"), P(("group", "tp"), "dp")),
        check_vma=False,
    )
```
